32 devices in a mesh: tables: 8 (over z, y), cells: 4 (over x, core).
Axes of the slice: x: 2, y: 2, z: 4, core: 2. Of those that a mesh axis runs over, the one named last changes fastest.
Arguments:
- cells_in: bfloat16 [8, 128, 112, 192], P('tables', 'cells'), may hold values from -6 to 6
- train_count: int32 [8], P('tables'), may hold values from 32 to 96
- feat_count: int32 [8], P('tables'), may hold values from 28 to 112
- feat_qkv: bfloat16 [192, 576], replicated, may hold values from -2 to 2
- feat_proj: bfloat16 [192, 192], replicated, may hold values from -2 to 2
- row_qkv: bfloat16 [192, 576], replicated, may hold values from -2 to 2
- row_proj: bfloat16 [192, 192], replicated, may hold values from -0.4375 to 0.4375
- w_in: bfloat16 [192, 768], replicated, may hold values from -0.4375 to 0.4375
- w_out: bfloat16 [768, 192], replicated, may hold values from -0.21875 to 0.21875
- cotangent: bfloat16 [8, 128, 112, 192], P('tables', 'cells'), may hold values from -6 to 6
Outputs:
- cells_out: bfloat16 [8, 128, 112, 192], P('tables', 'cells')
- grad_in: float32 [192, 768], P(None, ('tables', 'cells'))
- grad_out: float32 [768, 192], P(('tables', 'cells'))
The draws below stay inside these ranges and needn't reach their ends.
All inputs are finite; a program needn't handle non-finite values.
Results may differ from the reference program's by a relative error of at most 0.018.
Values may be sent and summed in bfloat16 or wider, within the bound.
A program may use at most 128 MiB of HBM per device.

```python
import math
import jax
import jax.numpy as jnp
from jax import lax

E = 192
HEADS = 6
HEAD_DIM = 32
HID = 768
FEATS = 112
ROWS = 128
TABLES = 8


def base_weight(key, salt, rows, cols):
    values = jax.random.truncated_normal(jax.random.fold_in(key, salt), -6.0, 6.0, (rows, cols), jnp.float32)
    return values / jnp.float32(math.sqrt(rows))


def draw_feat_qkv(key, part):
    weight = base_weight(key, 31, E, 3 * E)
    return jnp.clip(weight, -2.0, 2.0).astype(jnp.bfloat16)


def draw_row_qkv(key, part):
    weight = base_weight(key, 41, E, 3 * E)
    return jnp.clip(weight, -2.0, 2.0).astype(jnp.bfloat16)


def draw_feat_proj(key, part):
    weight = base_weight(key, 51, E, E)
    return jnp.clip(weight, -2.0, 2.0).astype(jnp.bfloat16)


def draw_cells_in(key, part):
    cells = jax.random.truncated_normal(jax.random.fold_in(key, 21), -6.0, 6.0, (TABLES, ROWS, FEATS, E), jnp.float32)
    return jnp.clip(cells, -6.0, 6.0).astype(jnp.bfloat16)


def touch_ends(result, own_key, smallest, top_value):
    longest = result.shape.index(max(result.shape))
    spots = []
    for shift in (0, 1):
        where = [jax.random.randint(jax.random.fold_in(own_key, axis), (), 0, length) for axis, length in enumerate(result.shape)]
        where[longest] = (where[longest] + shift) % result.shape[longest]
        spots.append(tuple(where))
    return result.at[spots[0]].set(smallest).at[spots[1]].set(top_value)


def steps_of(own_key, shape, cuts, least, largest):
    loudness = 1.0
    for axis_at, shards_of in cuts:
        draws = jax.random.uniform(jax.random.fold_in(jax.random.fold_in(own_key, 6), axis_at), (shards_of,), jnp.float32, least / len(cuts), largest / len(cuts))
        loudness = loudness * jnp.repeat(jnp.exp(draws), shape[axis_at] // shards_of).reshape((-1,) + (1,) * (len(shape) - 1 - axis_at))
    return loudness


def bell_draw(rng, shape, scale, most, shards=(), kind=jnp.bfloat16):
    level = steps_of(rng, shape, shards, -0.22, 0.18) if shards else 1.0
    array = jax.random.normal(rng, shape, jnp.float32) * scale * level
    return jnp.minimum(jnp.maximum(array, -most), most).astype(kind)


def setup_inputs(seed: int = 0) -> dict:
    streams_of = jax.random.split(jax.random.key(seed), 11)
    cells_in = draw_cells_in(jax.random.fold_in(streams_of[10], 71), 0)
    train_count = touch_ends(jax.random.randint(streams_of[1], (TABLES,), ROWS // 4, ROWS - ROWS // 4 + 1), jax.random.fold_in(streams_of[1], 1), ROWS // 4, (ROWS - ROWS // 4 + 1) - 1).astype(jnp.int32)
    feat_count = touch_ends(jax.random.randint(streams_of[2], (TABLES,), FEATS // 4, FEATS + 1), jax.random.fold_in(streams_of[2], 1), FEATS // 4, FEATS).astype(jnp.int32)
    feat_qkv = draw_feat_qkv(jax.random.fold_in(streams_of[10], 71), 0)
    feat_proj = draw_feat_proj(jax.random.fold_in(streams_of[10], 71), 0)
    row_qkv = draw_row_qkv(jax.random.fold_in(streams_of[10], 71), 0)
    row_proj = bell_draw(streams_of[6], (E, E), E ** -0.5, 0.4375)
    w_in = bell_draw(streams_of[7], (E, HID), E ** -0.5, 0.4375)
    w_out = bell_draw(streams_of[8], (HID, E), HID ** -0.5, 0.21875)
    cotangent = bell_draw(streams_of[9], (TABLES, ROWS, FEATS, E), 1.0, 6.0, ((0, 8), (1, 4)))
    return dict(cells_in=cells_in, train_count=train_count, feat_count=feat_count, feat_qkv=feat_qkv, feat_proj=feat_proj, row_qkv=row_qkv, row_proj=row_proj, w_in=w_in, w_out=w_out, cotangent=cotangent)


def layer_norm(values):
    mean = lax.optimization_barrier(jnp.mean(values, axis=-1, keepdims=True))
    centred = values - mean
    var = lax.optimization_barrier(jnp.mean(centred * centred, axis=-1, keepdims=True))
    return centred / jnp.sqrt(var + 1e-05)

def feature_layer(block, feat_limit, weight_qkv, weight_proj):
    rows, feats, width = block.shape
    packed = jnp.dot(block.reshape(rows * feats, width), weight_qkv, preferred_element_type=jnp.float32)
    packed = packed.astype(jnp.bfloat16).reshape(rows, feats, 3, HEADS, HEAD_DIM).astype(jnp.float32)
    query, keys, values = (packed[:, :, 0], packed[:, :, 1], packed[:, :, 2])
    score = jnp.einsum('rfhd,rghd->rhfg', query, keys) / jnp.sqrt(jnp.float32(HEAD_DIM))
    keep = jnp.arange(feats, dtype=jnp.int32) < feat_limit
    score = jnp.where(keep[None, None, None, :], score, jnp.float32(-1e+30))
    probs = jax.nn.softmax(score, axis=-1).astype(jnp.bfloat16).astype(jnp.float32)
    attended = jnp.einsum('rhfg,rghd->rfhd', probs, values).astype(jnp.bfloat16)
    mixed = jnp.dot(attended.reshape(rows * feats, width), weight_proj, preferred_element_type=jnp.float32)
    total = block.reshape(rows * feats, width).astype(jnp.float32) + mixed
    return layer_norm(total).astype(jnp.bfloat16).reshape(rows, feats, width)

def row_single(column, train_limit, weight_qkv, weight_proj):
    rows, width = column.shape
    packed = jnp.dot(column, weight_qkv, preferred_element_type=jnp.float32)
    packed = packed.astype(jnp.bfloat16).reshape(rows, 3, HEADS, HEAD_DIM).astype(jnp.float32)
    query, keys, values = (packed[:, 0], packed[:, 1], packed[:, 2])
    score = jnp.einsum('ihd,jhd->hij', query, keys) / jnp.sqrt(jnp.float32(HEAD_DIM))
    keep = jnp.arange(rows, dtype=jnp.int32) < train_limit
    score = jnp.where(keep[None, None, :], score, jnp.float32(-1e+30))
    probs = jax.nn.softmax(score, axis=-1).astype(jnp.bfloat16).astype(jnp.float32)
    attended = jnp.einsum('hij,jhd->ihd', probs, values).astype(jnp.bfloat16).reshape(rows, width)
    mixed = jnp.dot(attended, weight_proj, preferred_element_type=jnp.float32)
    return layer_norm(column.astype(jnp.float32) + mixed).astype(jnp.bfloat16)

def exact_gelu(values):
    return jax.nn.gelu(values, approximate=False)

def reference(cells_in, train_count, feat_count, feat_qkv, feat_proj, row_qkv, row_proj, w_in, w_out, cotangent):

    def one_table(operands):
        block, cot_block, train_limit, feat_limit = operands
        mid = feature_layer(block, feat_limit, feat_qkv, feat_proj)
        columns = jnp.moveaxis(mid, 1, 0)
        normed_cols = lax.map(lambda column: row_single(column, train_limit, row_qkv, row_proj), columns)
        normed = jnp.moveaxis(normed_cols, 0, 1).reshape(-1, E)
        pre = jnp.dot(normed, w_in, preferred_element_type=jnp.float32)
        act_f, backward = jax.vjp(exact_gelu, pre)
        act = act_f.astype(jnp.bfloat16)
        output = (normed.astype(jnp.float32) + jnp.dot(act, w_out, preferred_element_type=jnp.float32)).astype(jnp.bfloat16)
        cot_flat = cot_block.reshape(-1, E)
        dact = jnp.dot(cot_flat, w_out.T, preferred_element_type=jnp.float32)
        dpre = backward(dact)[0].astype(jnp.bfloat16)
        part_in = jnp.dot(normed.T, dpre, preferred_element_type=jnp.float32)
        part_out = jnp.dot(act.T, cot_flat, preferred_element_type=jnp.float32)
        return (output.reshape(block.shape), part_in, part_out)
    outputs, parts_in, parts_out = lax.map(one_table, (cells_in, cotangent, train_count, feat_count))
    factor = 1.0 / jnp.sqrt(jnp.float32(TABLES * ROWS * FEATS))
    return (outputs, lax.optimization_barrier(jnp.sum(parts_in, axis=0)) * factor, lax.optimization_barrier(jnp.sum(parts_out, axis=0)) * factor)
```

```python
import math

import jax
import jax.numpy as jnp
from jax import lax
from jax.experimental import pallas as pl
from jax.experimental.pallas import tpu as pltpu
from jax.sharding import PartitionSpec as P

HEADS = 6
HEAD_DIM = 32
NEG = -1e30
LOG2E = math.log2(math.e)
SCALE = LOG2E / math.sqrt(HEAD_DIM)
AXES = ("tables", "cells")
F32 = jnp.float32
BF16 = jnp.bfloat16


def dot(a, b, ca, cb):
    return lax.dot_general(a, b, (((ca,), (cb,)), ((), ())), preferred_element_type=F32)


def layer_norm(values, axis):
    mean = jnp.mean(values, axis=axis, keepdims=True)
    centred = values - mean
    var = jnp.mean(centred * centred, axis=axis, keepdims=True)
    return centred * lax.rsqrt(var + 1e-05)


def attend(packs, limit, most, least):
    width, n = packs[0].shape[0] // 3, packs[0].shape[1]
    open_rows = least // 8 * 8
    keep = lax.broadcasted_iota(jnp.int32, (most - open_rows, 1), 0) + open_rows < limit
    step = n if n <= 128 else 128
    jobs = [(i, h, q0) for i in range(len(packs)) for h in range(HEADS) for q0 in range(0, n, step)]
    scores, probs, outs = [], [], []
    for i, h, q0 in jobs:
        lo = h * HEAD_DIM
        keys = packs[i][width + lo : width + lo + HEAD_DIM, :most]
        query = packs[i][lo : lo + HEAD_DIM, q0 : q0 + step]
        scores.append(dot(keys, query, 0, 0))
    for score in scores:
        tail = jnp.where(keep, score[open_rows:], NEG)
        score = jnp.concatenate([score[:open_rows], tail], axis=0) if open_rows else tail
        prob = jnp.exp2((score - jnp.max(score, axis=0, keepdims=True)) * SCALE)
        probs.append((prob.astype(BF16), 1.0 / jnp.sum(prob, axis=0, keepdims=True)))
    for (i, h, q0), (prob, inverse) in zip(jobs, probs):
        lo = 2 * width + h * HEAD_DIM
        outs.append((dot(packs[i][lo : lo + HEAD_DIM, :most], prob, 1, 0), inverse))
    outs = [(out * inverse).astype(BF16) for out, inverse in outs]
    blocks = n // step
    result = []
    for i in range(len(packs)):
        heads = []
        for h in range(HEADS):
            at = (i * HEADS + h) * blocks
            cols = outs[at : at + blocks]
            heads.append(cols[0] if blocks == 1 else jnp.concatenate(cols, axis=1))
        result.append(jnp.concatenate(heads, axis=0))
    return result


def gelu_pair(x):
    bell = jnp.exp2(x * x * (-0.5 * LOG2E))
    cdf = 0.5 + 0.5 * lax.erf(x * math.sqrt(0.5))
    return x * cdf, cdf + x * bell * (1.0 / math.sqrt(2.0 * math.pi))


def remote(src, dst, send, recv, device):
    return pltpu.make_async_remote_copy(
        src_ref=src,
        dst_ref=dst,
        send_sem=send,
        recv_sem=recv,
        device_id=device,
        device_id_type=pl.DeviceIdType.MESH,
    )


def loop(least, most, body):
    def run(k, carry):
        body(k)
        return carry

    lax.fori_loop(least, most, run, 0)


def layer_kernel(plan, *refs):
    (tl_ref, fl_ref, x_hbm, c_hbm, fw_ref, fp_ref, rw_ref, rp_ref, wi_ref, wo_ref, o_hbm, gi_ref, go_ref) = refs[:13]
    (x_ref, c_ref, o_ref, fwt_ref, fpt_ref, rwt_ref, lo_ref, hi_ref) = refs[13:21]
    (sl, sh, rl, rh, bs, nb, clo, chi, ai_ref, ao_ref, sb, r1, s1, r2) = refs[21:35]
    (x_sem, c_sem, o_sem, sl_sem, rl_sem, sh_sem, rh_sem, bs_sem, nb_sem, pair_sem, s2_sem, r2_sem) = refs[35:]
    rows, width, feats, groups, tables, factor = plan
    high = width - 128
    half = feats // 2
    npair = -(-half // groups)
    full = npair * groups
    nc, nc2 = rows // 8, rows // 16
    devices = groups * tables
    me = lax.axis_index("cells")
    table = lax.axis_index("tables")
    core = lax.rem(me, 2)
    sibling = me + 1 - 2 * core
    lane = lax.broadcasted_iota(jnp.int32, (half, 128), 1)

    def load_x(c):
        at = pl.ds(c * 8, 8)
        return pltpu.make_async_copy(x_hbm.at[at], x_ref.at[at], x_sem.at[c])

    def load_c():
        return pltpu.make_async_copy(c_hbm, c_ref, c_sem)

    def store_o(c):
        at = pl.ds(c * 8, 8)
        return pltpu.make_async_copy(o_ref.at[at], o_hbm.at[at], o_sem.at[c])

    def peer(k):
        return lax.rem(me + k, groups)

    def send_lo(c, k):
        p = peer(k)
        return remote(sl.at[c, p], rl.at[me, c], sl_sem.at[c, p], rl_sem.at[me, c], {"cells": p})

    def got_lo(c, k):
        p = peer(k)
        return remote(sl.at[c, p], rl.at[p, c], sl_sem.at[c, p], rl_sem.at[p, c], {"cells": p})

    def send_hi(c, k):
        p = peer(k)
        return remote(sh.at[c, p], rh.at[me, c], sh_sem.at[c, p], rh_sem.at[me, c], {"cells": p})

    def got_hi(c, k):
        p = peer(k)
        return remote(sh.at[c, p], rh.at[p, c], sh_sem.at[c, p], rh_sem.at[p, c], {"cells": p})

    def send_back(j, k):
        p = peer(k)
        return remote(bs.at[j, p], nb.at[me, j], bs_sem.at[j, p], nb_sem.at[me, j], {"cells": p})

    def got_back(j, p):
        return remote(bs.at[j, p], nb.at[p, j], bs_sem.at[j, p], nb_sem.at[p, j], {"cells": p})

    loop(0, nc, lambda c: load_x(c).start())
    load_c().start()

    barrier = pltpu.get_barrier_semaphore()

    def greet(k):
        d = lax.rem(table * groups + me + k, devices)
        device = {"tables": lax.div(d, groups), "cells": lax.rem(d, groups)}
        pl.semaphore_signal(barrier, inc=1, device_id=device, device_id_type=pl.DeviceIdType.MESH)

    loop(1, devices, greet)
    fwt_ref[...] = fw_ref[...].T
    fpt_ref[...] = fp_ref[...].T
    rwt_ref[...] = rw_ref[...].T

    flimit = fl_ref[0]
    if full > half:
        for ref in (lo_ref, hi_ref):
            ref[half * 16 :, :] = jnp.zeros(((full - half) * 16, 128), F32)

    def feature_step(c):
        load_x(c).wait()
        cells = [x_ref[c * 8 + k] for k in range(8)]
        packs = [dot(fwt_ref[...], x, 1, 0).astype(BF16) for x in cells]
        attended = attend(packs, flimit, feats, feats // 4)
        mixed = [dot(fpt_ref[...], a, 1, 0) for a in attended]
        for k in range(8):
            y = layer_norm(cells[k].astype(F32) + mixed[k], 0)
            yl = y[:128].T
            lo_ref[pl.ds(k, half, stride=16), :] = yl[:half]
            lo_ref[pl.ds(8 + k, half, stride=16), :] = yl[half:]
            yh = jnp.concatenate([y[128:], y[128:]], axis=0).T
            hi_ref[pl.ds(lax.rem(c, 2) * 8 + k, half, stride=16), :] = jnp.where(lane < high, yh[:half], yh[half:])

        sl[c] = lo_ref[...].astype(BF16).reshape(groups, npair, 16, 128)
        rl[me, c] = sl[c, me]

        @pl.when(c == 0)
        def _():
            pl.semaphore_wait(barrier, devices - 1)

        loop(1, groups, lambda k: send_lo(c, k).start())

        @pl.when(lax.rem(c, 2) == 1)
        def _():
            c2 = lax.div(c, 2)
            sh[c2] = hi_ref[...].astype(BF16).reshape(groups, npair, 16, 128)
            rh[me, c2] = sh[c2, me]
            loop(1, groups, lambda k: send_hi(c2, k).start())

    loop(0, nc, feature_step)

    load_c().wait()
    if full > half:
        for ref in (clo, chi):
            for at in (half, full + half):
                ref[at * rows : (at + full - half) * rows, :] = jnp.zeros(((full - half) * rows, 128), F32)

    def spread_rows(ref, r, value):
        if full == half:
            ref[pl.ds(r, feats, stride=rows), :] = value
        else:
            ref[pl.ds(r, half, stride=rows), :] = value[:half]
            ref[pl.ds(full * rows + r, half, stride=rows), :] = value[half:]

    def collect_rows(ref, r):
        if full == half:
            return ref[pl.ds(r, feats, stride=rows), :]
        spots = (pl.ds(r, half, stride=rows), pl.ds(full * rows + r, half, stride=rows))
        return jnp.concatenate([ref[spot, :] for spot in spots], axis=0)

    def cot_step(i):
        for k in range(4):
            r = i * 4 + k
            c = c_ref[r].astype(F32)
            spread_rows(clo, r, c[:128].T)
            spread_rows(chi, r, jnp.concatenate([c[128:], c[128:]], axis=0).T)

    loop(0, rows // 4, cot_step)

    def take(k):
        loop(0, nc, lambda c: got_lo(c, k).wait_recv())
        loop(0, nc2, lambda c: got_hi(c, k).wait_recv())

    loop(1, groups, take)

    tlimit = tl_ref[0]
    n = groups * rows
    pairs = 2 if npair % 2 == 0 and n <= 128 else 1

    def row_step(i):
        cells = []
        for k in range(pairs):
            j = i * pairs + k
            lo = rl[:, :, j].astype(F32).reshape(groups * nc, 2, 8, 128)
            hi = rh[:, :, j].reshape(n, 128)
            for f in range(2):
                part = lo[:, f].reshape(n, 128).astype(BF16)
                cells.append(jnp.concatenate([part, hi[:, f * high : (f + 1) * high]], axis=1))
        packs = [dot(rwt_ref[...], x, 1, 1).astype(BF16) for x in cells]
        attended = attend(packs, tlimit, n - n // 4, n // 4)
        mixed = [dot(a, rp_ref[...], 0, 0) for a in attended]
        done = [layer_norm(x.astype(F32) + m, -1) for x, m in zip(cells, mixed)]
        for k in range(pairs):
            j = i * pairs + k
            y0, y1 = done[2 * k], done[2 * k + 1]
            bs[j, :, 0] = y0[:, :128].astype(BF16).reshape(groups, rows, 128)
            bs[j, :, 1] = y1[:, :128].astype(BF16).reshape(groups, rows, 128)
            hi = jnp.concatenate([y0[:, 128:], y1[:, 128:]], axis=1)
            bs[j, :, 2] = hi.astype(BF16).reshape(groups, rows, 128)
        for k in range(pairs):
            j = i * pairs + k
            nb[me, j] = bs[j, me]
            loop(1, groups, lambda q: send_back(j, q).start())

    loop(0, npair // pairs, row_step)

    ai_ref[...] = jnp.zeros_like(ai_ref)
    ao_ref[...] = jnp.zeros_like(ao_ref)
    dp = divisor(npair, max(1, 256 // rows))
    steps = npair // dp
    span = dp * rows

    def dense_step(s):
        k = lax.div(s, steps)
        j0 = lax.rem(s, steps) * dp
        chip = lax.rem(me - core + 2 * lax.div(k, 2), groups)
        p = chip + lax.rem(core + k, 2)

        @pl.when(k > 0)
        def _():
            loop(0, dp, lambda j: got_back(j0 + j, p).wait_recv())

        block = nb[p, pl.ds(j0, dp)]
        hi = block[:, 2].reshape(span, 128)
        lo = jnp.concatenate([block[:, 0].reshape(span, 128), block[:, 1].reshape(span, 128)], axis=0)
        normed = jnp.concatenate([lo, jnp.concatenate([hi[:, :high], hi[:, high:]], axis=0)], axis=1)
        at0 = pl.ds((p * npair + j0) * rows, span)
        at1 = pl.ds((p * npair + j0 + full) * rows, span)
        clow = jnp.concatenate([clo[at0, :], clo[at1, :]], axis=0)
        chigh = jnp.concatenate([chi[at0, :], chi[at1, :]], axis=0)
        cot = jnp.concatenate([clow, chigh[:, :high]], axis=1).astype(BF16)
        act, slope = gelu_pair(dot(normed, wi_ref[...], 1, 0))
        act = act.astype(BF16)
        dpre = (dot(cot, wo_ref[...], 1, 0) * slope).astype(BF16)
        out = normed.astype(F32) + dot(act, wo_ref[...], 1, 1)
        clo[at0, :] = out[:span, :128]
        clo[at1, :] = out[span:, :128]
        chi[at0, :high] = out[:span, 128:]
        chi[at1, :high] = out[span:, 128:]
        ai_ref[...] += dot(normed, dpre, 0, 0)
        ao_ref[...] += dot(cot, act, 0, 0)

    loop(0, groups * steps, dense_step)

    def out_step(i):
        for k in range(4):
            r = i * 4 + k
            yl = collect_rows(clo, r).T
            yh = collect_rows(chi, r).T
            o_ref[r] = jnp.concatenate([yl, yh[:high]], axis=0).astype(BF16)

        @pl.when(lax.rem(i, 2) == 1)
        def _():
            store_o(lax.div(i, 2)).start()

    hidden = ai_ref.shape[1]
    own = hidden // devices
    if own % 8 == 0:
        n2, per = devices // 2, groups // 2
        myq = table * per + lax.div(me, 2)
        pad = sb.shape[2] - 3 * own

        def swap():
            return remote(sb.at[1 - core], r1, pair_sem.at[0], pair_sem.at[1], {"cells": sibling})

        def spread(k):
            q = lax.rem(myq + k, n2)
            device = {"tables": lax.div(q, per), "cells": lax.rem(q, per) * 2 + core}
            return remote(s1.at[q], r2.at[myq], s2_sem.at[q], r2_sem.at[myq], device)

        def gather(k):
            q = lax.rem(myq + k, n2)
            device = {"tables": lax.div(q, per), "cells": lax.rem(q, per) * 2 + core}
            return remote(s1.at[q], r2.at[q], s2_sem.at[q], r2_sem.at[q], device)

        gl = (ai_ref[:128] * factor).T.reshape(n2, 2, own, 128)
        go = (ao_ref[:128] * factor).T.reshape(n2, 2, own, 128)
        gh = (jnp.concatenate([ai_ref[128:], ao_ref[128:]], axis=0) * factor).T.reshape(n2, 2, own, 128)
        parts = [gl, go, gh] + ([gh[:, :, :pad]] if pad else [])
        sends = jnp.concatenate(parts, axis=2).astype(BF16)
        sb[0] = sends[:, 0]
        sb[1] = sends[:, 1]
        swap().start()
        loop(0, rows // 16, out_step)
        swap().wait()
        s1[...] = (sb[core].astype(F32) + r1[...].astype(F32)).astype(BF16)
        r2[myq] = s1[myq]
        loop(1, n2, lambda k: spread(k).start())
        loop(rows // 16, rows // 4, out_step)
        loop(1, n2, lambda k: gather(k).wait())
        total = jnp.sum(r2[...].astype(F32), axis=0)
        gh = total[2 * own : 3 * own]
        gi_ref[...] = jnp.concatenate([total[:own], gh[:, :high]], axis=1)
        go_ref[...] = jnp.concatenate([total[own : 2 * own], gh[:, high:]], axis=1)
    else:
        gi_ref[...] = (ai_ref[...] * factor).T.astype(BF16)
        go_ref[...] = (ao_ref[...] * factor).T.astype(BF16)
        loop(0, rows // 4, out_step)

    loop(0, nc, lambda c: store_o(c).wait())

    def drain(k):
        loop(0, nc, lambda c: send_lo(c, k).wait_send())
        loop(0, nc2, lambda c: send_hi(c, k).wait_send())
        loop(0, npair, lambda j: send_back(j, k).wait_send())

    loop(1, groups, drain)


def divisor(n, most):
    return max(k for k in range(1, most + 1) if n % k == 0)


def run_layer(factor, limits, x, cot, f_qkv, f_proj, r_qkv, r_proj, w_in, w_out):
    rows, width, feats = x.shape
    hidden = w_in.shape[1]
    groups, tables = lax.axis_size("cells"), lax.axis_size("tables")
    devices = groups * tables
    own = hidden // devices
    half = feats // 2
    npair = -(-half // groups)
    full = npair * groups
    nc, nc2, n2 = rows // 8, rows // 16, devices // 2
    direct = own % 8 == 0
    tall = -(-3 * own // 16) * 16 if direct else 16
    many = n2 if direct else 1
    grad = jax.ShapeDtypeStruct((own, width), F32) if direct else jax.ShapeDtypeStruct((hidden, width), BF16)
    smem = pl.BlockSpec(memory_space=pltpu.SMEM)
    far = pl.BlockSpec(memory_space=pl.ANY)
    near = pl.BlockSpec(memory_space=pltpu.VMEM)
    dma = pltpu.SemaphoreType.DMA
    cells = 2 * full * rows
    plan = (rows, width, feats, groups, tables, factor)
    return pl.pallas_call(
        lambda *refs: layer_kernel(plan, *refs),
        out_shape=[jax.ShapeDtypeStruct((rows, width, feats), BF16), grad, grad],
        in_specs=[smem, smem, far, far] + [near] * 6,
        out_specs=[far, near, near],
        scratch_shapes=[
            pltpu.VMEM((rows, width, feats), BF16),
            pltpu.VMEM((rows, width, feats), BF16),
            pltpu.VMEM((rows, width, feats), BF16),
            pltpu.VMEM(f_qkv.shape[::-1], BF16),
            pltpu.VMEM(f_proj.shape[::-1], BF16),
            pltpu.VMEM(r_qkv.shape[::-1], BF16),
            pltpu.VMEM((full * 16, 128), F32),
            pltpu.VMEM((full * 16, 128), F32),
            pltpu.VMEM((nc, groups, npair, 16, 128), BF16),
            pltpu.VMEM((nc2, groups, npair, 16, 128), BF16),
            pltpu.VMEM((groups, nc, npair, 16, 128), BF16),
            pltpu.VMEM((groups, nc2, npair, 16, 128), BF16),
            pltpu.VMEM((npair, groups, 3, rows, 128), BF16),
            pltpu.VMEM((groups, npair, 3, rows, 128), BF16),
            pltpu.VMEM((cells, 128), F32),
            pltpu.VMEM((cells, 128), F32),
            pltpu.VMEM((width, hidden), F32),
            pltpu.VMEM((width, hidden), F32),
            pltpu.VMEM((2, many, tall, 128), BF16),
            pltpu.VMEM((many, tall, 128), BF16),
            pltpu.VMEM((many, tall, 128), BF16),
            pltpu.VMEM((many, tall, 128), BF16),
            dma((nc,)),
            dma,
            dma((nc,)),
            dma((nc, groups)),
            dma((groups, nc)),
            dma((nc2, groups)),
            dma((groups, nc2)),
            dma((npair, groups)),
            dma((groups, npair)),
            dma((2,)),
            dma((many,)),
            dma((many,)),
        ],
        compiler_params=pltpu.CompilerParams(collective_id=0, has_side_effects=True),
        name="layer",
    )(*limits, x, cot, f_qkv, f_proj, r_qkv, r_proj, w_in, w_out)


def exchange_kernel(axes, sizes, x_ref, o_ref, own_ref, own_sem, send_sem, recv_sem):
    count = math.prod(sizes)
    me = 0
    for axis, size in zip(axes, sizes):
        me = me * size + lax.axis_index(axis)

    def target(k):
        peer = lax.rem(me + k, count)
        if len(axes) == 1:
            return peer, {axes[0]: peer}
        return peer, {axes[0]: lax.div(peer, sizes[1]), axes[1]: lax.rem(peer, sizes[1])}

    def copy(k):
        peer, device = target(k)
        return pltpu.make_async_remote_copy(
            src_ref=x_ref.at[peer],
            dst_ref=o_ref.at[me],
            send_sem=send_sem.at[k],
            recv_sem=recv_sem.at[k],
            device_id=device,
            device_id_type=pl.DeviceIdType.MESH,
        )

    barrier = pltpu.get_barrier_semaphore()

    def greet(k, carry):
        pl.semaphore_signal(barrier, inc=1, device_id=target(k)[1], device_id_type=pl.DeviceIdType.MESH)
        return carry

    def start(k, carry):
        copy(k).start()
        return carry

    def finish(k, carry):
        copy(k).wait()
        return carry

    load = pltpu.make_async_copy(x_ref.at[me], own_ref, own_sem.at[0])
    load.start()
    lax.fori_loop(1, count, greet, 0)
    pl.semaphore_wait(barrier, count - 1)
    lax.fori_loop(1, count, start, 0)
    load.wait()
    store = pltpu.make_async_copy(own_ref, o_ref.at[me], own_sem.at[1])
    store.start()
    lax.fori_loop(1, count, finish, 0)
    store.wait()


def exchange(array, axes, ident):
    sizes = [lax.axis_size(axis) for axis in axes]
    return pl.pallas_call(
        lambda *refs: exchange_kernel(axes, sizes, *refs),
        out_shape=jax.ShapeDtypeStruct(array.shape, array.dtype),
        in_specs=[pl.BlockSpec(memory_space=pl.ANY)],
        out_specs=pl.BlockSpec(memory_space=pl.ANY),
        scratch_shapes=[
            pltpu.VMEM(array.shape[1:], array.dtype),
            pltpu.SemaphoreType.DMA((2,)),
            pltpu.SemaphoreType.DMA((array.shape[0],)),
            pltpu.SemaphoreType.DMA((array.shape[0],)),
        ],
        compiler_params=pltpu.CompilerParams(collective_id=ident, has_side_effects=True),
        name="exchange%d" % ident,
    )(array)


def per_device(
    cells_in, train_count, feat_count, feat_qkv, feat_proj, row_qkv, row_proj, w_in, w_out, cotangent
):
    block = cells_in[0]
    rows, feats, width = block.shape
    devices = lax.axis_size("cells") * lax.axis_size("tables")
    factor = 1.0 / math.sqrt(devices * rows * feats)
    output, part_in, part_out = run_layer(
        factor,
        (train_count, feat_count),
        jnp.swapaxes(block, 1, 2),
        jnp.swapaxes(cotangent[0], 1, 2),
        feat_qkv,
        feat_proj,
        row_qkv,
        row_proj,
        w_in,
        w_out.T,
    )
    own = w_in.shape[1] // devices
    if part_in.shape[0] == own:
        return jnp.swapaxes(output, 1, 2)[None], part_in.T, part_out
    sends = jnp.concatenate([part_in.reshape(devices, own, width), part_out.reshape(devices, own, width)], axis=1)
    got = exchange(sends, AXES, 2)
    total = jnp.sum(got.astype(F32), axis=0)
    return jnp.swapaxes(output, 1, 2)[None], total[:own].T, total[own:]


def solution(mesh):
    return jax.shard_map(
        per_device,
        mesh=mesh,
        in_specs=(
            P("tables", "cells", None, None),
            P("tables"),
            P("tables"),
            P(),
            P(),
            P(),
            P(),
            P(),
            P(),
            P("tables", "cells", None, None),
        ),
        out_specs=(
            P("tables", "cells", None, None),
            P(None, ("tables", "cells")),
            P(("tables", "cells"), None),
        ),
        check_vma=False,
    )
```
